32 devices in a mesh: dp: 8 (over y, x, core), tensor: 4 (over z).
Axes of the slice: x: 2, y: 2, z: 4, core: 2. Of those that a mesh axis runs over, the one named last changes fastest.
Arguments:
- tokens: bfloat16 [8, 1024, 1152], P('dp', 'tensor'), may hold values from -6 to 6
- labels: int32 [8], P('dp'), may hold values from 0 to 1000
- timesteps: int32 [8], P('dp'), may hold values from 0 to 999
- label_table: bfloat16 [1001, 1152], replicated, may hold values from -6 to 6
- ada_weight: bfloat16 [1152, 6912], P(None, 'tensor'), may hold values from -0.1875 to 0.1875
- ada_bias: float32 [6912], P('tensor'), may hold values from 0.5 to 1.5
- qkv_weight: bfloat16 [3, 1152, 1152], P(None, None, 'tensor'), may hold values from -0.09375 to 0.09375
- qv_bias: float32 [2, 1152], P(None, 'tensor'), may hold values from -3 to 3
- proj_weight: bfloat16 [1152, 1152], P('tensor'), may hold values from -2 to 2
- out_bias: float32 [2, 1152], replicated, may hold values from -3 to 3
- fc1_weight: bfloat16 [1152, 4608], P(None, 'tensor'), may hold values from -0.1875 to 0.1875
- fc1_bias: float32 [4608], P('tensor'), may hold values from -3 to 3
- fc2_weight: bfloat16 [4608, 1152], P('tensor'), may hold values from -0.09375 to 0.09375
- cotangent: bfloat16 [8, 1024, 1152], P('dp', 'tensor'), may hold values from -6 to 6
Outputs:
- output: bfloat16 [8, 1024, 1152], P('dp', 'tensor')
- input_grad: float32 [8, 1024, 1152], P('dp', 'tensor')
- table_grad: float32 [1001, 1152], replicated
- ada_weight_grad: float32 [1152, 6912], P('dp', 'tensor')
- ada_bias_grad: float32 [6912], P(('tensor', 'dp'))
- qkv_weight_grad: float32 [3, 1152, 1152], P(None, 'dp', 'tensor')
- qv_bias_grad: float32 [2, 1152], replicated
- proj_weight_grad: float32 [1152, 1152], P('tensor', 'dp')
- out_bias_grad: float32 [2, 1152], replicated
- fc1_weight_grad: float32 [1152, 4608], P('dp', 'tensor')
- fc1_bias_grad: float32 [4608], P(('tensor', 'dp'))
- fc2_weight_grad: float32 [4608, 1152], P('tensor', 'dp')
The draws below stay inside these ranges and needn't reach their ends.
All inputs are finite; a program needn't handle non-finite values.
Results may differ from the reference program's by a relative error of at most 0.018.
Values may be sent and summed in bfloat16 or wider, within the bound.
A program may use at most 192 MiB of HBM per device.

```python
import math
import jax
import jax.numpy as jnp
from jax import lax

D = 1152
HEADS = 16
HEAD_DIM = 72
FF = 4608
CLASSES = 1001
SEQ = 1024
LATENTS = 8
N_TENSOR = 4


def place_ends(drawn, rng, least, high):
    dims = drawn.shape
    spot = [jax.random.randint(jax.random.fold_in(rng, axis), (), 0, dims[axis]) for axis in range(len(dims))]
    drawn = drawn.at[tuple(spot)].set(least)
    longest = dims.index(max(dims))
    spot[longest] = (spot[longest] + 1) % dims[longest]
    return drawn.at[tuple(spot)].set(high)


def spiked(values, stream_key, source, target, blocks, factor):
    def block_of(dim):
        return (jnp.arange(values.shape[dim]) // (values.shape[dim] // blocks)).reshape((-1,) + (1,) * (values.ndim - 1 - dim))

    one_side = jax.random.permutation(stream_key, blocks)[block_of(target)]
    far = (block_of(target) + blocks // 2) % blocks
    return jnp.where((block_of(source) == one_side) | (block_of(source) == far), factor * values, values)


def block_levels(rng, dims, cuts, low, top_value):
    def one(axis_at, blocks):
        draws = jax.random.uniform(jax.random.fold_in(jax.random.fold_in(rng, 6), axis_at), (blocks,), jnp.float32, low / len(cuts), top_value / len(cuts))
        return jnp.repeat(jnp.exp(draws), dims[axis_at] // blocks).reshape((-1,) + (1,) * (len(dims) - axis_at - 1))

    loudness = one(*cuts[0])
    for cut in cuts[1:]:
        loudness = loudness * one(*cut)
    return loudness


def scatter_about(key, dims, deviation, bound, pieces=(), held_as=jnp.bfloat16):
    values = jax.random.normal(key, dims, jnp.float32) * deviation
    if len(pieces) > 0:
        values = block_levels(key, dims, pieces, -0.22, 0.18) * values
    return jnp.clip(values, min=-bound, max=bound).astype(held_as)


def noise_with(own_key, extent, width, most, cuts, heavy, held_as=jnp.bfloat16):
    entries = width * jax.random.normal(own_key, extent, jnp.float32)
    if cuts:
        entries = entries * block_levels(own_key, extent, cuts, -0.22, 0.18)
    return jnp.clip(spiked(entries, jax.random.fold_in(own_key, 3), *heavy), -most, most).astype(held_as)


def setup_inputs(seed: int = 0) -> dict:
    splits = jax.random.split(jax.random.key(seed), 15)
    tokens = noise_with(splits[0], (LATENTS, SEQ, D), 1.0, 6.0, ((0, 8), (1, 4)), (0, 2, 8, 2.0))
    labels = place_ends(jax.random.randint(splits[1], (LATENTS,), 0, CLASSES), jax.random.fold_in(splits[1], 1), 0, CLASSES - 1).astype(jnp.int32)
    timesteps = place_ends(jax.random.randint(splits[2], (LATENTS,), 0, 1000), jax.random.fold_in(splits[2], 1), 0, 999).astype(jnp.int32)
    label_table = scatter_about(splits[3], (CLASSES, D), 1.0, 6.0)
    ada_weight = scatter_about(splits[4], (D, 6 * D), D ** -0.5, 0.1875, ((1, 4),))
    ada_bias = jnp.clip(0.5 + 1.0 * jax.random.uniform(splits[5], (6 * D,), jnp.float32) ** block_levels(splits[5], (6 * D,), ((0, 4),), -0.2, 0.2), 0.5, 1.5)
    qkv_weight = scatter_about(splits[6], (3, D, D), (4 * D) ** -0.5, 0.09375, ((2, 4),))
    qv_bias = scatter_about(splits[7], (2, D), 0.5, 3.0, ((1, 4),), jnp.float32)
    proj_weight = scatter_about(splits[8], (D, D), (HEAD_DIM // 8) ** -0.5, 2.0, ((0, 4),))
    out_bias = scatter_about(splits[9], (2, D), 0.5, 3.0, (), jnp.float32)
    fc1_weight = scatter_about(splits[10], (D, FF), D ** -0.5, 0.1875, ((1, 4),))
    fc1_bias = scatter_about(splits[11], (FF,), 0.5, 3.0, ((0, 4),), jnp.float32)
    fc2_weight = scatter_about(splits[12], (FF, D), FF ** -0.5, 0.09375, ((0, 4),))
    cotangent = noise_with(splits[13], (LATENTS, SEQ, D), 1.0, 6.0, ((0, 8), (1, 4)), (0, 2, 8, 2.0))
    return dict(tokens=tokens, labels=labels, timesteps=timesteps, label_table=label_table, ada_weight=ada_weight, ada_bias=ada_bias, qkv_weight=qkv_weight, qv_bias=qv_bias, proj_weight=proj_weight, out_bias=out_bias, fc1_weight=fc1_weight, fc1_bias=fc1_bias, fc2_weight=fc2_weight, cotangent=cotangent)


@jax.custom_vjp
def low(v):
    return lax.optimization_barrier(v.astype(jnp.bfloat16)).astype(jnp.float32)

@jax.custom_vjp
def low_back(v):
    return v

def low_keep(v):
    return (low(v), None)

def low_pass(kept, grad):
    return (grad,)

def back_keep(v):
    return (v, None)

def back_low(kept, grad):
    return (low(grad),)
low.defvjp(low_keep, low_pass)
low_back.defvjp(back_keep, back_low)
highest = lax.Precision.HIGHEST

def time_features(timesteps):
    half = D // 2
    freqs = jnp.exp(-math.log(10000.0) * jnp.arange(half, dtype=jnp.float32) / half)
    angles = timesteps.astype(jnp.float32)[:, None] * freqs[None, :]
    return jnp.concatenate([jnp.cos(angles), jnp.sin(angles)], axis=1)

def normalize(values):
    center = values - lax.optimization_barrier(jnp.mean(values, axis=-1, keepdims=True))
    spread = lax.optimization_barrier(jnp.mean(center * center, axis=-1, keepdims=True))
    return center * lax.rsqrt(spread + 1e-06)

def layer(params, tokens_one, label, temb_one):
    table, ada_w, ada_b, qkv_w, qv_b, proj_w, out_b, fc1_w, fc1_b, fc2_w = params
    cond = table[label] + temb_one
    cond_low = low(jax.nn.silu(cond))
    modulation = jnp.dot(cond_low, ada_w, precision=highest) + ada_b
    shift_attn, scale_attn, gate_attn, shift_mlp, scale_mlp, gate_mlp = jnp.split(modulation, 6)
    attn_input = low(normalize(tokens_one) * (1.0 + scale_attn) + shift_attn)
    query = low(low_back(jnp.dot(attn_input, qkv_w[0], precision=highest) + qv_b[0]))
    keyset = low(low_back(jnp.dot(attn_input, qkv_w[1], precision=highest)))
    valset = low(low_back(jnp.dot(attn_input, qkv_w[2], precision=highest) + qv_b[1]))
    query = query.reshape(SEQ, HEADS, HEAD_DIM)
    keyset = keyset.reshape(SEQ, HEADS, HEAD_DIM)
    valset = valset.reshape(SEQ, HEADS, HEAD_DIM)
    scores = low_back(jnp.einsum('qhd,khd->hqk', query, keyset, precision=highest) / math.sqrt(HEAD_DIM))
    probs_low = low(jax.nn.softmax(scores, axis=-1))
    attn_mix = low(low_back(jnp.einsum('hqk,khd->qhd', probs_low, valset, precision=highest).reshape(SEQ, D)))
    group = D // N_TENSOR
    parts = jnp.einsum('sgc,gcd->gsd', attn_mix.reshape(SEQ, N_TENSOR, group), proj_w.reshape(N_TENSOR, group, D), precision=highest)
    attn_branch = low_back(lax.optimization_barrier(jnp.sum(low(parts), axis=0))) + out_b[0]
    middle = tokens_one + gate_attn * attn_branch
    mlp_input = low(normalize(middle) * (1.0 + scale_mlp) + shift_mlp)
    pre_act = low_back(jnp.dot(mlp_input, fc1_w, precision=highest) + fc1_b)
    hidden = low(jax.nn.gelu(pre_act, approximate=True))
    hgroup = FF // N_TENSOR
    mparts = jnp.einsum('sgc,gcd->gsd', hidden.reshape(SEQ, N_TENSOR, hgroup), fc2_w.reshape(N_TENSOR, hgroup, D), precision=highest)
    mlp_branch = low_back(lax.optimization_barrier(jnp.sum(low(mparts), axis=0))) + out_b[1]
    return middle + gate_mlp * mlp_branch

def reference(tokens, labels, timesteps, label_table, ada_weight, ada_bias, qkv_weight, qv_bias, proj_weight, out_bias, fc1_weight, fc1_bias, fc2_weight, cotangent):
    params = tuple((p.astype(jnp.float32) for p in (label_table, ada_weight, ada_bias, qkv_weight, qv_bias, proj_weight, out_bias, fc1_weight, fc1_bias, fc2_weight)))
    temb = time_features(timesteps)
    zeros = jax.tree.map(jnp.zeros_like, params)

    def visit(totals, item):
        tokens_one, label, temb_one, cot_one = item
        out_one, pull = jax.vjp(lambda prm, tok: layer(prm, tok, label, temb_one), params, tokens_one)
        grads, token_grad = pull(cot_one)
        totals = jax.tree.map(jnp.add, totals, grads)
        return (totals, (out_one.astype(jnp.bfloat16), token_grad))
    totals, (output, input_grad) = lax.scan(visit, zeros, (tokens.astype(jnp.float32), labels, temb, cotangent.astype(jnp.float32)))
    table_grad, ada_weight_grad, ada_bias_grad, qkv_weight_grad, qv_bias_grad, proj_weight_grad, out_bias_grad, fc1_weight_grad, fc1_bias_grad, fc2_weight_grad = totals
    return (output, input_grad, table_grad, ada_weight_grad, ada_bias_grad, qkv_weight_grad, qv_bias_grad, proj_weight_grad, out_bias_grad, fc1_weight_grad, fc1_bias_grad, fc2_weight_grad)
```

```python
import math

import jax
import jax.numpy as jnp
from jax import lax
from jax.sharding import PartitionSpec as P

HEAD_DIM = 72
SEQ = 1024


highest = lax.Precision.HIGHEST


def time_features(timesteps, width):
    half = width // 2
    freqs = jnp.exp(-math.log(10000.0) * jnp.arange(half, dtype=jnp.float32) / half)
    angles = timesteps.astype(jnp.float32)[:, None] * freqs[None, :]
    return jnp.concatenate([jnp.cos(angles), jnp.sin(angles)], axis=1)


def normalize(values):
    center = values - jnp.mean(values, axis=-1, keepdims=True)
    spread = jnp.mean(center * center, axis=-1, keepdims=True)
    inv_std = lax.rsqrt(spread + 1e-06)
    return (center * inv_std, inv_std)


def norm_back(grad, normed, inv_std):
    mean_grad = jnp.mean(grad, axis=-1, keepdims=True)
    mean_proj = jnp.mean(grad * normed, axis=-1, keepdims=True)
    return (grad - mean_grad - normed * mean_proj) * inv_std


def body(
    tokens,
    labels,
    timesteps,
    label_table,
    ada_weight,
    ada_bias,
    qkv_weight,
    qv_bias,
    proj_weight,
    out_bias,
    fc1_weight,
    fc1_bias,
    fc2_weight,
    cotangent,
):
    latent_count = tokens.shape[0]
    width = tokens.shape[2]
    tensor_rank = lax.axis_index("tensor")
    head_cols = qkv_weight.shape[2]
    local_heads = head_cols // HEAD_DIM
    block_rows = min(512, SEQ)
    block_count = SEQ // block_rows
    inv_root = 1.0 / math.sqrt(HEAD_DIM)
    cond = label_table[labels].astype(jnp.float32) + time_features(timesteps, width)
    cond_low = jax.nn.silu(cond).astype(jnp.bfloat16)
    mod_part = jnp.dot(cond_low, ada_weight, preferred_element_type=jnp.float32) + ada_bias
    modulation = lax.all_gather(mod_part, "tensor", axis=1, tiled=True)
    shift_attn, scale_attn, gate_attn, shift_mlp, scale_mlp, gate_mlp = [
        piece[:, None, :] for piece in jnp.split(modulation, 6, axis=1)
    ]
    normed_one, inv_one = normalize(tokens.astype(jnp.float32))
    attn_input = (normed_one * (1.0 + scale_attn) + shift_attn).astype(jnp.bfloat16)
    attn_rows = lax.all_gather(attn_input, "tensor", axis=1, tiled=True)
    query = (
        jnp.einsum("lsd,dc->lsc", attn_rows, qkv_weight[0], preferred_element_type=jnp.float32)
        + qv_bias[0]
    ).astype(jnp.bfloat16)
    keyset = jnp.einsum(
        "lsd,dc->lsc", attn_rows, qkv_weight[1], preferred_element_type=jnp.float32
    ).astype(jnp.bfloat16)
    valset = (
        jnp.einsum("lsd,dc->lsc", attn_rows, qkv_weight[2], preferred_element_type=jnp.float32)
        + qv_bias[1]
    ).astype(jnp.bfloat16)
    head_shape = (latent_count, SEQ, local_heads, HEAD_DIM)
    query_heads = query.reshape(head_shape)
    key_heads = keyset.reshape(head_shape)
    val_heads = valset.reshape(head_shape)

    def attend(index):
        start = index * block_rows
        query_block = lax.dynamic_slice_in_dim(query_heads, start, block_rows, axis=1)
        scores = (
            jnp.einsum(
                "lqhd,lkhd->lhqk", query_block, key_heads, preferred_element_type=jnp.float32
            )
            * inv_root
        )
        peak = jnp.max(scores, axis=-1, keepdims=True)
        expd = jnp.exp(scores - peak)
        total = jnp.sum(expd, axis=-1, keepdims=True)
        probs_low = (expd / total).astype(jnp.bfloat16)
        log_total = peak[..., 0] + jnp.log(total[..., 0])
        mixed_block = jnp.einsum(
            "lhqk,lkhd->lqhd", probs_low, val_heads, preferred_element_type=jnp.float32
        ).astype(jnp.bfloat16)
        return (mixed_block, log_total)

    mixed_blocks, log_totals = lax.map(attend, jnp.arange(block_count, dtype=jnp.int32))
    attn_mix = jnp.moveaxis(mixed_blocks, 0, 1).reshape(latent_count, SEQ, head_cols)
    attn_terms = jnp.einsum(
        "lsc,cd->lsd", attn_mix, proj_weight, preferred_element_type=jnp.float32
    )
    attn_branch = (
        lax.psum_scatter(
            attn_terms.astype(jnp.bfloat16), "tensor", scatter_dimension=1, tiled=True
        ).astype(jnp.float32)
        + out_bias[0]
    )
    middle = tokens.astype(jnp.float32) + gate_attn * attn_branch
    normed_two, inv_two = normalize(middle)
    mlp_input = (normed_two * (1.0 + scale_mlp) + shift_mlp).astype(jnp.bfloat16)
    mlp_rows = lax.all_gather(mlp_input, "tensor", axis=1, tiled=True)
    pre_act = (
        jnp.einsum("lsd,dc->lsc", mlp_rows, fc1_weight, preferred_element_type=jnp.float32)
        + fc1_bias
    )
    hidden = jax.nn.gelu(pre_act, approximate=True).astype(jnp.bfloat16)
    mlp_terms = jnp.einsum("lsc,cd->lsd", hidden, fc2_weight, preferred_element_type=jnp.float32)
    mlp_branch = (
        lax.psum_scatter(
            mlp_terms.astype(jnp.bfloat16), "tensor", scatter_dimension=1, tiled=True
        ).astype(jnp.float32)
        + out_bias[1]
    )
    output = (middle + gate_mlp * mlp_branch).astype(jnp.bfloat16)
    out_grad = cotangent.astype(jnp.float32)
    mlp_grad = gate_mlp * out_grad
    gate_mlp_grad = jnp.sum(out_grad * mlp_branch, axis=1)
    mlp_bias_grad = jnp.sum(mlp_grad, axis=(0, 1))
    mlp_grad_rows = lax.all_gather(mlp_grad.astype(jnp.bfloat16), "tensor", axis=1, tiled=True)
    hidden_grad = jnp.einsum(
        "lsd,cd->lsc", mlp_grad_rows, fc2_weight, preferred_element_type=jnp.float32
    )
    unused_value, gelu_pull = jax.vjp(lambda value: jax.nn.gelu(value, approximate=True), pre_act)
    pre_grad = gelu_pull(hidden_grad)[0].astype(jnp.bfloat16)
    fc2_grad = jnp.einsum("lsc,lsd->cd", hidden, mlp_grad_rows, preferred_element_type=jnp.float32)
    fc1_grad = jnp.einsum("lsd,lsc->dc", mlp_rows, pre_grad, preferred_element_type=jnp.float32)
    fc1_bias_grad = jnp.sum(pre_grad, axis=(0, 1), dtype=jnp.float32)
    mlp_back_terms = jnp.einsum(
        "lsc,dc->lsd", pre_grad, fc1_weight, preferred_element_type=jnp.float32
    )
    mlp_back = lax.psum_scatter(
        mlp_back_terms.astype(jnp.bfloat16), "tensor", scatter_dimension=1, tiled=True
    ).astype(jnp.float32)
    shift_mlp_grad = jnp.sum(mlp_back, axis=1)
    scale_mlp_grad = jnp.sum(mlp_back * normed_two, axis=1)
    middle_grad = out_grad + norm_back(mlp_back * (1.0 + scale_mlp), normed_two, inv_two)
    attn_grad = gate_attn * middle_grad
    gate_attn_grad = jnp.sum(middle_grad * attn_branch, axis=1)
    attn_bias_grad = jnp.sum(attn_grad, axis=(0, 1))
    attn_grad_rows = lax.all_gather(attn_grad.astype(jnp.bfloat16), "tensor", axis=1, tiled=True)
    proj_grad = jnp.einsum(
        "lsc,lsd->cd", attn_mix, attn_grad_rows, preferred_element_type=jnp.float32
    )
    mix_grad = jnp.einsum(
        "lsd,cd->lsc", attn_grad_rows, proj_weight, preferred_element_type=jnp.float32
    ).astype(jnp.bfloat16)
    mix_heads = mix_grad.reshape(head_shape)

    def attend_back(carry, index):
        key_total, val_total = carry
        start = index * block_rows
        query_block = lax.dynamic_slice_in_dim(query_heads, start, block_rows, axis=1)
        mix_block = lax.dynamic_slice_in_dim(mix_heads, start, block_rows, axis=1)
        scores = (
            jnp.einsum(
                "lqhd,lkhd->lhqk", query_block, key_heads, preferred_element_type=jnp.float32
            )
            * inv_root
        )
        probs = jnp.exp(scores - log_totals[index][..., None])
        prob_grad = jnp.einsum(
            "lqhd,lkhd->lhqk", mix_block, val_heads, preferred_element_type=jnp.float32
        )
        row_dot = jnp.sum(probs * prob_grad, axis=-1, keepdims=True)
        score_grad = (probs * (prob_grad - row_dot)).astype(jnp.bfloat16)
        query_block_grad = (
            jnp.einsum("lhqk,lkhd->lqhd", score_grad, key_heads, preferred_element_type=jnp.float32)
            * inv_root
        ).astype(jnp.bfloat16)
        key_total = (
            key_total
            + jnp.einsum(
                "lhqk,lqhd->lkhd", score_grad, query_block, preferred_element_type=jnp.float32
            )
            * inv_root
        )
        val_total = val_total + jnp.einsum(
            "lhqk,lqhd->lkhd",
            probs.astype(jnp.bfloat16),
            mix_block,
            preferred_element_type=jnp.float32,
        )
        return ((key_total, val_total), query_block_grad)

    empty = jnp.zeros(head_shape, jnp.float32)
    (key_total, val_total), query_blocks = lax.scan(
        attend_back, (empty, empty), jnp.arange(block_count, dtype=jnp.int32)
    )
    query_grad = jnp.moveaxis(query_blocks, 0, 1).reshape(latent_count, SEQ, head_cols)
    key_grad = key_total.reshape(latent_count, SEQ, head_cols).astype(jnp.bfloat16)
    val_grad = val_total.reshape(latent_count, SEQ, head_cols).astype(jnp.bfloat16)
    qkv_grad = jnp.stack(
        [
            jnp.einsum("lsd,lsc->dc", attn_rows, grad_item, preferred_element_type=jnp.float32)
            for grad_item in (query_grad, key_grad, val_grad)
        ]
    )
    qv_local = jnp.stack(
        [
            jnp.sum(query_grad, axis=(0, 1), dtype=jnp.float32),
            jnp.sum(val_grad, axis=(0, 1), dtype=jnp.float32),
        ]
    )
    attn_back_terms = (
        jnp.einsum("lsc,dc->lsd", query_grad, qkv_weight[0], preferred_element_type=jnp.float32)
        + jnp.einsum("lsc,dc->lsd", key_grad, qkv_weight[1], preferred_element_type=jnp.float32)
        + jnp.einsum("lsc,dc->lsd", val_grad, qkv_weight[2], preferred_element_type=jnp.float32)
    )
    attn_back = lax.psum_scatter(
        attn_back_terms.astype(jnp.bfloat16), "tensor", scatter_dimension=1, tiled=True
    ).astype(jnp.float32)
    shift_attn_grad = jnp.sum(attn_back, axis=1)
    scale_attn_grad = jnp.sum(attn_back * normed_one, axis=1)
    input_grad = middle_grad + norm_back(attn_back * (1.0 + scale_attn), normed_one, inv_one)
    mod_part_grad = jnp.concatenate(
        [
            shift_attn_grad,
            scale_attn_grad,
            gate_attn_grad,
            shift_mlp_grad,
            scale_mlp_grad,
            gate_mlp_grad,
        ],
        axis=1,
    )
    col_count = ada_weight.shape[1]
    mod_grad = lax.psum_scatter(mod_part_grad, "tensor", scatter_dimension=1, tiled=True)
    small = jnp.concatenate([mod_grad, cond, labels.astype(jnp.float32)[:, None]], axis=1)
    every = lax.all_gather(small, "dp", axis=0, tiled=True)
    mod_all, cond_all, label_all = (
        every[:, :col_count],
        every[:, col_count : col_count + width],
        every[:, col_count + width].astype(jnp.int32),
    )
    low_all = jax.nn.silu(cond_all).astype(jnp.bfloat16).astype(jnp.float32)
    dp_rank, dp_size = lax.axis_index("dp"), lax.axis_size("dp")
    row_count = width // dp_size
    low_rows = lax.dynamic_slice_in_dim(low_all, dp_rank * row_count, row_count, 1)
    ada_part = jnp.dot(low_rows.T, mod_all, precision=highest)
    bias_count = col_count // dp_size
    ada_bias_part = lax.dynamic_slice_in_dim(
        jnp.sum(mod_all, axis=0), dp_rank * bias_count, bias_count, 0
    )
    silu_terms = jnp.dot(mod_all, ada_weight.astype(jnp.float32).T, precision=highest)
    qv_full = lax.dynamic_update_slice_in_dim(
        jnp.zeros((2, width), jnp.float32), qv_local, tensor_rank * head_cols, 1
    )
    out_bias_part = jnp.stack([attn_bias_grad, mlp_bias_grad])
    silu_grad = lax.psum(silu_terms, "tensor")
    out_bias_grad, qv_bias_grad = lax.psum((out_bias_part, qv_full), ("dp", "tensor"))
    unused_cond, silu_pull = jax.vjp(jax.nn.silu, cond_all)
    cond_grad = silu_pull(silu_grad)[0]
    class_ids = jnp.arange(label_table.shape[0], dtype=jnp.int32)
    one_hot = (label_all[:, None] == class_ids[None, :]).astype(jnp.float32)
    table_grad = jnp.dot(one_hot.T, cond_grad, precision=highest)
    qkv_part, proj_part, fc1_part, fc2_part, fc1_bias_part = (
        lax.psum_scatter(qkv_grad, "dp", scatter_dimension=1, tiled=True),
        lax.psum_scatter(proj_grad, "dp", scatter_dimension=1, tiled=True),
        lax.psum_scatter(fc1_grad, "dp", scatter_dimension=0, tiled=True),
        lax.psum_scatter(fc2_grad, "dp", scatter_dimension=1, tiled=True),
        lax.psum_scatter(fc1_bias_grad, "dp", scatter_dimension=0, tiled=True),
    )
    return (
        output,
        input_grad,
        table_grad,
        ada_part,
        ada_bias_part,
        qkv_part,
        qv_bias_grad,
        proj_part,
        out_bias_grad,
        fc1_part,
        fc1_bias_part,
        fc2_part,
    )


def solution(mesh):
    placed = (
        P("dp", "tensor", None),
        P("dp"),
        P("dp"),
        P(),
        P(None, "tensor"),
        P("tensor"),
        P(None, None, "tensor"),
        P(None, "tensor"),
        P("tensor", None),
        P(),
        P(None, "tensor"),
        P("tensor"),
        P("tensor", None),
        P("dp", "tensor", None),
    )
    return jax.shard_map(
        body,
        mesh=mesh,
        in_specs=placed,
        out_specs=(
            P("dp", "tensor", None),
            P("dp", "tensor", None),
            P(),
            P("dp", "tensor"),
            P(("tensor", "dp")),
            P(None, "dp", "tensor"),
            P(),
            P("tensor", "dp"),
            P(),
            P("dp", "tensor"),
            P(("tensor", "dp")),
            P("tensor", "dp"),
        ),
        check_vma=False,
    )
```

```python
import math

import jax
import jax.numpy as jnp
from jax import lax
from jax.experimental import pallas as pl
from jax.experimental.pallas import tpu as pltpu
from jax.sharding import PartitionSpec as P

HEAD_DIM = 72
SEQ = 1024


highest = lax.Precision.HIGHEST


def time_features(timesteps, width):
    half = width // 2
    freqs = jnp.exp(-math.log(10000.0) * jnp.arange(half, dtype=jnp.float32) / half)
    angles = timesteps.astype(jnp.float32)[:, None] * freqs[None, :]
    return jnp.concatenate([jnp.cos(angles), jnp.sin(angles)], axis=1)


def normalize(values):
    center = values - jnp.mean(values, axis=-1, keepdims=True)
    spread = jnp.mean(center * center, axis=-1, keepdims=True)
    inv_std = lax.rsqrt(spread + 1e-06)
    return (center * inv_std, inv_std)


def norm_back(grad, normed, inv_std):
    mean_grad = jnp.mean(grad, axis=-1, keepdims=True)
    mean_proj = jnp.mean(grad * normed, axis=-1, keepdims=True)
    return (grad - mean_grad - normed * mean_proj) * inv_std


def body(
    tokens,
    labels,
    timesteps,
    label_table,
    ada_weight,
    ada_bias,
    qkv_weight,
    qv_bias,
    proj_weight,
    out_bias,
    fc1_weight,
    fc1_bias,
    fc2_weight,
    cotangent,
):
    latent_count = tokens.shape[0]
    width = tokens.shape[2]
    tensor_rank = lax.axis_index("tensor")
    head_cols = qkv_weight.shape[2]
    local_heads = head_cols // HEAD_DIM
    block_rows = min(512, SEQ)
    block_count = SEQ // block_rows
    inv_root = 1.0 / math.sqrt(HEAD_DIM)
    cond = label_table[labels].astype(jnp.float32) + time_features(timesteps, width)
    cond_low = jax.nn.silu(cond).astype(jnp.bfloat16)
    mod_part = jnp.dot(cond_low, ada_weight, preferred_element_type=jnp.float32) + ada_bias
    modulation = lax.all_gather(mod_part, "tensor", axis=1, tiled=True)
    shift_attn, scale_attn, gate_attn, shift_mlp, scale_mlp, gate_mlp = [
        piece[:, None, :] for piece in jnp.split(modulation, 6, axis=1)
    ]
    normed_one, inv_one = normalize(tokens.astype(jnp.float32))
    attn_input = (normed_one * (1.0 + scale_attn) + shift_attn).astype(jnp.bfloat16)
    attn_rows = lax.all_gather(attn_input, "tensor", axis=1, tiled=True)
    query = (
        jnp.einsum("lsd,dc->lsc", attn_rows, qkv_weight[0], preferred_element_type=jnp.float32)
        + qv_bias[0]
    ).astype(jnp.bfloat16)
    keyset = jnp.einsum(
        "lsd,dc->lsc", attn_rows, qkv_weight[1], preferred_element_type=jnp.float32
    ).astype(jnp.bfloat16)
    valset = (
        jnp.einsum("lsd,dc->lsc", attn_rows, qkv_weight[2], preferred_element_type=jnp.float32)
        + qv_bias[1]
    ).astype(jnp.bfloat16)
    head_shape = (latent_count, SEQ, local_heads, HEAD_DIM)
    query_heads = query.reshape(head_shape)
    key_heads = keyset.reshape(head_shape)
    val_heads = valset.reshape(head_shape)

    def attend(index):
        start = index * block_rows
        query_block = lax.dynamic_slice_in_dim(query_heads, start, block_rows, axis=1)
        scores = (
            jnp.einsum(
                "lqhd,lkhd->lhqk", query_block, key_heads, preferred_element_type=jnp.float32
            )
            * inv_root
        )
        peak = jnp.max(scores, axis=-1, keepdims=True)
        expd = jnp.exp(scores - peak)
        total = jnp.sum(expd, axis=-1, keepdims=True)
        probs_low = (expd / total).astype(jnp.bfloat16)
        log_total = peak[..., 0] + jnp.log(total[..., 0])
        mixed_block = jnp.einsum(
            "lhqk,lkhd->lqhd", probs_low, val_heads, preferred_element_type=jnp.float32
        ).astype(jnp.bfloat16)
        return (mixed_block, log_total)

    mixed_blocks, log_totals = lax.map(attend, jnp.arange(block_count, dtype=jnp.int32))
    attn_mix = jnp.moveaxis(mixed_blocks, 0, 1).reshape(latent_count, SEQ, head_cols)
    attn_terms = jnp.einsum(
        "lsc,cd->lsd", attn_mix, proj_weight, preferred_element_type=jnp.float32
    )
    attn_branch = (
        lax.psum_scatter(
            attn_terms.astype(jnp.bfloat16), "tensor", scatter_dimension=1, tiled=True
        ).astype(jnp.float32)
        + out_bias[0]
    )
    middle = tokens.astype(jnp.float32) + gate_attn * attn_branch
    normed_two, inv_two = normalize(middle)
    mlp_input = (normed_two * (1.0 + scale_mlp) + shift_mlp).astype(jnp.bfloat16)
    mlp_rows = lax.all_gather(mlp_input, "tensor", axis=1, tiled=True)
    pre_act = (
        jnp.einsum("lsd,dc->lsc", mlp_rows, fc1_weight, preferred_element_type=jnp.float32)
        + fc1_bias
    )
    hidden = jax.nn.gelu(pre_act, approximate=True).astype(jnp.bfloat16)
    mlp_terms = jnp.einsum("lsc,cd->lsd", hidden, fc2_weight, preferred_element_type=jnp.float32)
    mlp_branch = (
        lax.psum_scatter(
            mlp_terms.astype(jnp.bfloat16), "tensor", scatter_dimension=1, tiled=True
        ).astype(jnp.float32)
        + out_bias[1]
    )
    output = (middle + gate_mlp * mlp_branch).astype(jnp.bfloat16)
    out_grad = cotangent.astype(jnp.float32)
    mlp_grad = gate_mlp * out_grad
    gate_mlp_grad = jnp.sum(out_grad * mlp_branch, axis=1)
    mlp_bias_grad = jnp.sum(mlp_grad, axis=(0, 1))
    mlp_grad_rows = lax.all_gather(mlp_grad.astype(jnp.bfloat16), "tensor", axis=1, tiled=True)
    hidden_grad = jnp.einsum(
        "lsd,cd->lsc", mlp_grad_rows, fc2_weight, preferred_element_type=jnp.float32
    )
    unused_value, gelu_pull = jax.vjp(lambda value: jax.nn.gelu(value, approximate=True), pre_act)
    pre_grad = gelu_pull(hidden_grad)[0].astype(jnp.bfloat16)
    fc2_grad = jnp.einsum("lsc,lsd->cd", hidden, mlp_grad_rows, preferred_element_type=jnp.float32)
    fc1_grad = jnp.einsum("lsd,lsc->dc", mlp_rows, pre_grad, preferred_element_type=jnp.float32)
    fc1_bias_grad = jnp.sum(pre_grad, axis=(0, 1), dtype=jnp.float32)
    mlp_back_terms = jnp.einsum(
        "lsc,dc->lsd", pre_grad, fc1_weight, preferred_element_type=jnp.float32
    )
    mlp_back = lax.psum_scatter(
        mlp_back_terms.astype(jnp.bfloat16), "tensor", scatter_dimension=1, tiled=True
    ).astype(jnp.float32)
    shift_mlp_grad = jnp.sum(mlp_back, axis=1)
    scale_mlp_grad = jnp.sum(mlp_back * normed_two, axis=1)
    middle_grad = out_grad + norm_back(mlp_back * (1.0 + scale_mlp), normed_two, inv_two)
    attn_grad = gate_attn * middle_grad
    gate_attn_grad = jnp.sum(middle_grad * attn_branch, axis=1)
    attn_bias_grad = jnp.sum(attn_grad, axis=(0, 1))
    attn_grad_rows = lax.all_gather(attn_grad.astype(jnp.bfloat16), "tensor", axis=1, tiled=True)
    proj_grad = jnp.einsum(
        "lsc,lsd->cd", attn_mix, attn_grad_rows, preferred_element_type=jnp.float32
    )
    mix_grad = jnp.einsum(
        "lsd,cd->lsc", attn_grad_rows, proj_weight, preferred_element_type=jnp.float32
    ).astype(jnp.bfloat16)
    mix_heads = mix_grad.reshape(head_shape)

    def attend_back(carry, index):
        key_total, val_total = carry
        start = index * block_rows
        query_block = lax.dynamic_slice_in_dim(query_heads, start, block_rows, axis=1)
        mix_block = lax.dynamic_slice_in_dim(mix_heads, start, block_rows, axis=1)
        scores = (
            jnp.einsum(
                "lqhd,lkhd->lhqk", query_block, key_heads, preferred_element_type=jnp.float32
            )
            * inv_root
        )
        probs = jnp.exp(scores - log_totals[index][..., None])
        prob_grad = jnp.einsum(
            "lqhd,lkhd->lhqk", mix_block, val_heads, preferred_element_type=jnp.float32
        )
        row_dot = jnp.sum(probs * prob_grad, axis=-1, keepdims=True)
        score_grad = (probs * (prob_grad - row_dot)).astype(jnp.bfloat16)
        query_block_grad = (
            jnp.einsum("lhqk,lkhd->lqhd", score_grad, key_heads, preferred_element_type=jnp.float32)
            * inv_root
        ).astype(jnp.bfloat16)
        key_total = (
            key_total
            + jnp.einsum(
                "lhqk,lqhd->lkhd", score_grad, query_block, preferred_element_type=jnp.float32
            )
            * inv_root
        )
        val_total = val_total + jnp.einsum(
            "lhqk,lqhd->lkhd",
            probs.astype(jnp.bfloat16),
            mix_block,
            preferred_element_type=jnp.float32,
        )
        return ((key_total, val_total), query_block_grad)

    empty = jnp.zeros(head_shape, jnp.float32)
    (key_total, val_total), query_blocks = lax.scan(
        attend_back, (empty, empty), jnp.arange(block_count, dtype=jnp.int32)
    )
    query_grad = jnp.moveaxis(query_blocks, 0, 1).reshape(latent_count, SEQ, head_cols)
    key_grad = key_total.reshape(latent_count, SEQ, head_cols).astype(jnp.bfloat16)
    val_grad = val_total.reshape(latent_count, SEQ, head_cols).astype(jnp.bfloat16)
    qkv_grad = jnp.stack(
        [
            jnp.einsum("lsd,lsc->dc", attn_rows, grad_item, preferred_element_type=jnp.float32)
            for grad_item in (query_grad, key_grad, val_grad)
        ]
    )
    qv_local = jnp.stack(
        [
            jnp.sum(query_grad, axis=(0, 1), dtype=jnp.float32),
            jnp.sum(val_grad, axis=(0, 1), dtype=jnp.float32),
        ]
    )
    attn_back_terms = (
        jnp.einsum("lsc,dc->lsd", query_grad, qkv_weight[0], preferred_element_type=jnp.float32)
        + jnp.einsum("lsc,dc->lsd", key_grad, qkv_weight[1], preferred_element_type=jnp.float32)
        + jnp.einsum("lsc,dc->lsd", val_grad, qkv_weight[2], preferred_element_type=jnp.float32)
    )
    attn_back = lax.psum_scatter(
        attn_back_terms.astype(jnp.bfloat16), "tensor", scatter_dimension=1, tiled=True
    ).astype(jnp.float32)
    shift_attn_grad = jnp.sum(attn_back, axis=1)
    scale_attn_grad = jnp.sum(attn_back * normed_one, axis=1)
    input_grad = middle_grad + norm_back(attn_back * (1.0 + scale_attn), normed_one, inv_one)
    mod_part_grad = jnp.concatenate(
        [
            shift_attn_grad,
            scale_attn_grad,
            gate_attn_grad,
            shift_mlp_grad,
            scale_mlp_grad,
            gate_mlp_grad,
        ],
        axis=1,
    )
    col_count = ada_weight.shape[1]
    mod_grad = lax.psum_scatter(mod_part_grad, "tensor", scatter_dimension=1, tiled=True)
    small = jnp.concatenate([mod_grad, cond, labels.astype(jnp.float32)[:, None]], axis=1)
    every = lax.all_gather(small, "dp", axis=0, tiled=True)
    mod_all, cond_all, label_all = (
        every[:, :col_count],
        every[:, col_count : col_count + width],
        every[:, col_count + width].astype(jnp.int32),
    )
    low_all = jax.nn.silu(cond_all).astype(jnp.bfloat16).astype(jnp.float32)
    dp_rank, dp_size = lax.axis_index("dp"), lax.axis_size("dp")
    row_count = width // dp_size
    low_rows = lax.dynamic_slice_in_dim(low_all, dp_rank * row_count, row_count, 1)
    ada_part = jnp.dot(low_rows.T, mod_all, precision=highest)
    bias_count = col_count // dp_size
    ada_bias_part = lax.dynamic_slice_in_dim(
        jnp.sum(mod_all, axis=0), dp_rank * bias_count, bias_count, 0
    )
    silu_terms = jnp.dot(mod_all, ada_weight.astype(jnp.float32).T, precision=highest)
    qv_full = lax.dynamic_update_slice_in_dim(
        jnp.zeros((2, width), jnp.float32), qv_local, tensor_rank * head_cols, 1
    )
    out_bias_part = jnp.stack([attn_bias_grad, mlp_bias_grad])
    silu_grad = lax.psum(silu_terms, "tensor")
    out_bias_grad, qv_bias_grad = lax.psum((out_bias_part, qv_full), ("dp", "tensor"))
    unused_cond, silu_pull = jax.vjp(jax.nn.silu, cond_all)
    cond_grad = silu_pull(silu_grad)[0]
    class_ids = jnp.arange(label_table.shape[0], dtype=jnp.int32)
    one_hot = (label_all[:, None] == class_ids[None, :]).astype(jnp.float32)
    table_grad = jnp.dot(one_hot.T, cond_grad, precision=highest)
    qkv_part, proj_part, fc1_part, fc2_part, fc1_bias_part = (
        lax.psum_scatter(qkv_grad, "dp", scatter_dimension=1, tiled=True),
        lax.psum_scatter(proj_grad, "dp", scatter_dimension=1, tiled=True),
        lax.psum_scatter(fc1_grad, "dp", scatter_dimension=0, tiled=True),
        lax.psum_scatter(fc2_grad, "dp", scatter_dimension=1, tiled=True),
        lax.psum_scatter(fc1_bias_grad, "dp", scatter_dimension=0, tiled=True),
    )
    return (
        output,
        input_grad,
        table_grad,
        ada_part,
        ada_bias_part,
        qkv_part,
        qv_bias_grad,
        proj_part,
        out_bias_grad,
        fc1_part,
        fc1_bias_part,
        fc2_part,
    )


MESH = pl.DeviceIdType.MESH
f32, bf16 = jnp.float32, jnp.bfloat16
LANES = 128


def dot(a, b, dims):
    return lax.dot_general(a, b, (dims, ((), ())), preferred_element_type=f32)


NN, NT, TN = ((1,), (0,)), ((1,), (1,)), ((0,), (0,))


class Spot:
    def __init__(self):
        self.dp, self.z = lax.axis_index("dp"), lax.axis_index("tensor")
        self.q, self.p, self.g = self.dp % 2, self.z % 2, self.z // 2
        self.c = (self.dp // 2) % 4
        self.rank = self.p + 2 * self.q
        self.home = self.q == self.g
        self.away = self.q != self.g
        self.sib = (self.flip(self.dp, 1), self.z)
        self.nbr = (self.dp, self.flip(self.z, 1))
        self.swap = (self.flip(self.dp, 1), self.flip(self.z, 2))
        self.peers = [(self.flip(self.dp, 2 * k), self.z) for k in (1, 2, 3)]
        self.r_sib, self.r_nbr, self.r_diag = (self.flip(self.rank, k) for k in (2, 1, 3))

    @staticmethod
    def flip(value, bits):
        return jnp.bitwise_xor(value, bits)


def send(src, dst, sems, i, dev):
    return pltpu.make_async_remote_copy(
        src_ref=src, dst_ref=dst, send_sem=sems.at[0, i], recv_sem=sems.at[1, i],
        device_id=dev, device_id_type=MESH,
    )


def quarter(rank, size=256):
    return pl.ds(pl.multiple_of(rank * size, size), size)


def loop(count, fn):
    def step(i, carry):
        fn(i)
        return carry
    lax.fori_loop(0, count, step, 0)


class Gather:
    def __init__(self, at, rows, sems, base):
        self.at, self.rows, self.sems, self.base = at, rows, sems, base

    def copy(self, rank, i, dev):
        block = self.rows.at[quarter(rank)]
        return send(block, block, self.sems, self.base + i, dev)

    def start(self):
        self.copy(self.at.rank, 0, self.at.nbr).start()
        self.copy(self.at.rank, 1, self.at.sib).start()

    def take_sib(self):
        self.copy(self.at.r_sib, 1, self.at.sib).wait_recv()

    def take_nbr(self):
        self.copy(self.at.r_nbr, 0, self.at.nbr).wait_recv()
        self.copy(self.at.r_nbr, 2, self.at.sib).start()

    def take_diag(self):
        self.copy(self.at.r_diag, 2, self.at.sib).wait_recv()

    def finish(self):
        self.copy(self.at.rank, 0, self.at.nbr).wait_send()
        self.copy(self.at.rank, 1, self.at.sib).wait_send()
        self.copy(self.at.r_nbr, 2, self.at.sib).wait_send()


class Scatter:
    def __init__(self, at, out, into, sems, base):
        self.at, self.out, self.into, self.sems, self.base = at, out, into, sems, base

    def copy(self, i):
        return send(self.out.at[i], self.into.at[i], self.sems, self.base + i,
                    self.at.nbr if i == 2 else self.at.sib)

    def start(self, i):
        self.copy(i).start()

    def take(self, i):
        self.copy(i).wait_recv()

    def finish(self):
        for i in range(3):
            self.copy(i).wait_send()


def entry(at, extra=()):
    barrier = pltpu.get_barrier_semaphore()
    mates = [at.sib, at.nbr, at.swap, *at.peers, *extra]
    for mate in mates:
        pl.semaphore_signal(barrier, inc=1, device_id=mate, device_id_type=MESH)
    pl.semaphore_wait(barrier, len(mates))


def center_rows(x):
    mean = jnp.mean(x, axis=1, keepdims=True)
    center = x - mean
    inv = lax.rsqrt(jnp.mean(center * center, axis=1, keepdims=True) + 1e-6)
    return center * inv, inv


def split_heads(acc_ref, store):
    lane = lax.broadcasted_iota(jnp.int32, (acc_ref.shape[0], LANES), 1)
    for h in range(4):
        tile, off = divmod(HEAD_DIM * h, LANES)
        two = acc_ref[:, tile * LANES:(tile + 2) * LANES] if tile < 2 else acc_ref[:, 128:384]
        if off:
            two = pltpu.roll(two, 2 * LANES - off, 1)
        store(h, jnp.where(lane < HEAD_DIM, two[:, :LANES], 0.0))


def join_heads(parts):
    rows = parts[0].shape[0]
    zero = jnp.zeros((rows, LANES), parts[0].dtype)
    tiles = [parts[0], zero, zero]
    for h in (1, 2, 3):
        tile, off = divmod(HEAD_DIM * h, LANES)
        two = pltpu.roll(jnp.concatenate([parts[h], zero], axis=1), off, 1)
        tiles[tile] = tiles[tile] + two[:, :LANES]
        if tile + 1 < 3:
            tiles[tile + 1] = tiles[tile + 1] + two[:, LANES:]
    return jnp.concatenate(tiles, axis=1)[:, :4 * HEAD_DIM]


GELU_A, GELU_B = math.sqrt(2.0 / math.pi), 0.044715

S_X, S_C, S_BIAS, S_MOD, S_AG1, S_AG2, S_AG3, S_AG4, S_RS1, S_RS3, S_RS2, S_W1, S_W2 = (
    0, 1, 2, 3, 7, 10, 13, 16, 19, 22, 25, 28, 38)
N_SEMS = 38 + 30


def kf(tok, cot, mblk, bblk, obias, wqkv, wproj, wfc1, wfc2,
       xr, qn, kn, vn, kt, lse, mix, gr, mgrad, xs, cs, mid, mods, stats, mlpown, mlpz, g1, g2, wq, wp,
       w1, w2, vt, mr, cr, hgrad, hid, pgr, rso, rsi, own, nbrf, rs2o, rs2i, n2, branch, mrecv, bias, acc, mixt, inv2,
       stage, sems, lsem):
    at = Spot()
    me = (at.dp, at.z)
    inv_root = 1.0 / math.sqrt(HEAD_DIM)
    entry(at, [(at.dp, at.flip(at.z, 2)), (at.dp, at.flip(at.z, 3)), (at.flip(at.dp, 1), at.flip(at.z, 1)),
               (at.flip(at.dp, 1), at.flip(at.z, 3))])
    weights = [(wqkv, wq, 288), (wproj, wp, 72), (wfc1, w1, 288), (wfc2, w2, 288)]

    def piece(i, slot, side):
        if i < 3:
            return weights[0][side].at[i, pl.ds(pl.multiple_of(slot * 288, 8), 288), :]
        if i == 3:
            return weights[1][side].at[pl.ds(pl.multiple_of(slot * 72, 8), 72), :]
        ref = weights[3 if i < 7 else 2][side]
        return ref.at[pl.ds(pl.multiple_of(slot * 288 + (i - 4) % 3 * 96, 8), 96), :]

    def import_first(i):
        return send(piece(i, at.c, 0), piece(i, at.c, 1), sems, S_W1 + i, at.swap)

    def import_next(i, k, slot):
        block = piece(i, slot, 1)
        return send(block, block, sems, S_W2 + 3 * i + k, at.peers[k])

    def import_start(*pieces):
        @pl.when(at.away)
        def _():
            for i in pieces:
                import_first(i).start()

    def import_hand_on(*pieces):
        @pl.when(at.away)
        def _():
            for i in pieces:
                import_first(i).wait_recv()
                for k in range(3):
                    import_next(i, k, at.c).start()

    def import_wait(j, *pieces):
        @pl.when(at.away)
        def _():
            for i in pieces:
                for k in range(3):
                    import_next(i, k, at.flip(at.c, k + 1)).wait_recv()

        @pl.when(at.home)
        def _():
            pltpu.make_async_copy(weights[j][0], weights[j][1], lsem.at[j]).wait()

    own_rows = quarter(at.rank)
    cown = cr.at[own_rows]

    @pl.when(at.away)
    def _():
        send(tok, xs, sems, S_X, at.swap).start()
        send(bblk, bias, sems, S_BIAS, at.swap).start()
        for i in (0, 1, 2):
            import_first(i).start()

    @pl.when(at.home)
    def _():
        pltpu.make_async_copy(tok, xs, sems.at[1, S_X]).start()
        pltpu.make_async_copy(bblk, bias, sems.at[1, S_BIAS]).start()
        pltpu.make_async_copy(cot, cown, sems.at[1, S_C]).start()
        for i in range(4):
            pltpu.make_async_copy(weights[i][0], weights[i][1], lsem.at[i]).start()

    def mod_copy(core, pp):
        dev = (at.dp - at.q + core, 2 * at.q + pp)
        return dev, send(mblk, mrecv.at[at.z], sems, S_MOD, dev)

    def for_mods(remote, local):
        for core in range(2):
            for pp in range(2):
                mine = (at.q == core) & (at.z == 2 * at.q + pp)
                dev = (at.dp - at.q + core, 2 * at.q + pp)
                cp = pltpu.make_async_remote_copy(
                    src_ref=mblk, dst_ref=mrecv.at[at.z], send_sem=sems.at[0, S_MOD + 2 * core + pp],
                    recv_sem=sems.at[1, S_MOD + at.z], device_id=dev, device_id_type=MESH)

                @pl.when(jnp.logical_not(mine))
                def _():
                    remote(cp)

                if local is not None:
                    @pl.when(mine)
                    def _():
                        local(pltpu.make_async_copy(mblk, mrecv.at[at.z], sems.at[1, S_MOD + at.z]))

    for_mods(lambda cp: cp.start(), lambda cp: cp.start())
    for k in range(4):
        pltpu.make_async_copy(mblk, mrecv.at[k], sems.at[1, S_MOD + k]).wait()
    lane = lax.broadcasted_iota(jnp.int32, (1, 1152), 1)
    rolled = [pltpu.roll(mrecv[k], 576, 1) for k in range(4)]
    for j in range(6):
        (ka, ia), (kb, ib) = divmod(2 * j, 3), divmod(2 * j + 1, 3)
        mods[j:j + 1, :] = jnp.where(lane < 576, mrecv[ka, ia:ia + 1, :], rolled[kb][ib:ib + 1, :])
    mods[6:8, :] = mrecv[0, 3:5, :]
    shift_attn, scale_attn, gate_attn, shift_mlp, scale_mlp, gate_mlp = (pl.ds(j, 1) for j in range(6))

    pltpu.make_async_copy(tok, xs, sems.at[1, S_X]).wait()

    def norm_one(i):
        rows = pl.ds(pl.multiple_of(i * 32, 32), 32)
        normed, _ = center_rows(xs[rows, :].astype(f32))
        target = pl.ds(pl.multiple_of(at.rank * 256 + i * 32, 32), 32)
        xr[target, :] = (normed * (1.0 + mods[scale_attn, :]) + mods[shift_attn, :]).astype(bf16)
    loop(8, norm_one)
    ag1 = Gather(at, xr, sems, S_AG1)
    ag1.start()
    pltpu.make_async_copy(bblk, bias, sems.at[1, S_BIAS]).wait()
    import_start(3)

    @pl.when(at.away)
    def _():
        send(cot, cr.at[quarter(at.r_sib)], sems, S_C, at.swap).start()
    import_start(4, 5, 6)
    import_hand_on(0, 1, 2)
    import_wait(0, 0, 1, 2)

    def slot_of(i):
        return at.flip(at.rank, ((i & 1) << 1) | (i >> 1))

    def qkv_block(i):
        @pl.when(i == 1)
        def _():
            ag1.take_sib()

        @pl.when(i == 2)
        def _():
            ag1.take_nbr()

        @pl.when(i == 3)
        def _():
            ag1.take_diag()
        rows = quarter(slot_of(i))
        x = xr[rows, :]
        for t, (nat, tra) in enumerate(((qn, None), (kn, kt), (vn, vt))):
            value = dot(x, wq[t], NN)
            if t != 1:
                value = value + bias[(1 if t == 0 else 2):(2 if t == 0 else 3), :288]
            acc[:, :288] = value

            def store(h, head):
                nat[h, rows, :] = head.astype(bf16)
                if tra is not None:
                    tra[h, :, rows] = head.T.astype(bf16)
            split_heads(acc, store)
    loop(4, qkv_block)
    ag1.finish()

    ag2 = Gather(at, cr, sems, S_AG2)
    import_hand_on(3)

    rs1 = Scatter(at, rso, rsi, sems, S_RS1)

    def attend_block(i):
        slot = at.flip(at.rank, 3 - (((i & 1) << 1) | (i >> 1)))
        rows = quarter(slot)

        def head(h):
            st = dot(kn[h], qn[h, rows, :], NT)
            peak = jnp.max(st, axis=0, keepdims=True)
            ex = jnp.exp((st - peak) * inv_root)
            total = jnp.sum(ex, axis=0, keepdims=True)
            probs = (ex * (1.0 / total)).astype(bf16)
            lse[h, :, rows] = jnp.broadcast_to(peak * inv_root + jnp.log(total), (8, 256))
            out = dot(vt[h], probs, NN)
            mixt[pl.ds(pl.multiple_of(h * HEAD_DIM, 8), HEAD_DIM), :] = out[:HEAD_DIM, :]
        loop(4, head)
        low = mixt[...].T[:, :288].astype(bf16)
        mix[rows, :] = low
        @pl.when(i == 0)
        def _():
            import_wait(1, 3)
        part = dot(low, wp[...], NN)

        @pl.when(i == 0)
        def _():
            rso[0] = part.astype(bf16)
            rs1.start(0)

        @pl.when(i == 1)
        def _():
            rs1.take(0)
            rso[2] = (part + rsi[0].astype(f32)).astype(bf16)
            rs1.start(2)
            pltpu.make_async_copy(cot, cown, sems.at[1, S_C]).wait()
            cs[...] = cown[...]
            ag2.start()
            import_start(7, 8, 9)

        @pl.when(i == 2)
        def _():
            rso[1] = part.astype(bf16)
            rs1.start(1)

        @pl.when(i == 3)
        def _():
            own[...] = part
            import_hand_on(4, 5, 6)
    mixt[288:, :] = jnp.zeros((96, 256), f32)
    loop(4, attend_block)
    ag2.take_sib()
    ag2.take_nbr()
    rs1.take(1)
    rs1.take(2)
    stats[...] = jnp.zeros(stats.shape, f32)

    def middle_rows(i):
        rows = pl.ds(pl.multiple_of(i * 32, 32), 32)
        br = own[rows, :] + rsi[1, rows, :].astype(f32) + rsi[2, rows, :].astype(f32) + obias[0:1, :]
        branch[rows, :] = br
        m = xs[rows, :].astype(f32) + mods[gate_attn, :] * br
        mid[rows, :] = m
        normed, inv = center_rows(m)
        n2[rows, :] = normed
        inv2[rows, :] = jnp.broadcast_to(inv, (32, LANES))
        target = pl.ds(pl.multiple_of(at.rank * 256 + i * 32, 32), 32)
        mr[target, :] = (normed * (1.0 + mods[scale_mlp, :]) + mods[shift_mlp, :]).astype(bf16)
    loop(8, middle_rows)
    rs1.finish()
    ag3 = Gather(at, mr, sems, S_AG3)
    ag3.start()

    ag2.take_diag()
    ag2.finish()
    import_wait(3, 4, 5, 6)
    import_hand_on(7, 8, 9)

    def gate_cot(i):
        rows = pl.ds(pl.multiple_of(i * 64, 64), 64)
        cr[rows, :] = (mods[gate_mlp, :] * cr[rows, :].astype(f32)).astype(bf16)
    loop(16, gate_cot)

    def hgrad_block(i):
        rows = quarter(i)
        hgrad[rows, :] = dot(cr[rows, :], w2[...], NT)
    loop(4, hgrad_block)
    import_wait(2, 7, 8, 9)
    rs3 = Scatter(at, rso, rsi, sems, S_RS3)

    def mlp_block(i):
        slot = slot_of(i)
        rows = quarter(slot)

        @pl.when(i == 1)
        def _():
            ag3.take_sib()

        @pl.when(i == 2)
        def _():
            ag3.take_nbr()

        @pl.when(i == 3)
        def _():
            ag3.take_diag()
        big[...] = dot(mr[rows, :], w1[...], NN)

        def act(j):
            sub = pl.ds(pl.multiple_of(j * 32, 32), 32)
            full = pl.ds(pl.multiple_of(slot * 256 + j * 32, 32), 32)
            v = big[sub, :] + bias[0:1, :]
            v2 = v * v
            t = jnp.tanh(GELU_A * (v + GELU_B * (v2 * v)))
            half = 0.5 * (1.0 + t)
            hid[full, :] = (v * half).astype(bf16)
            slope = half + 0.5 * v * (1.0 - t * t) * (GELU_A * (1.0 + 3.0 * GELU_B * v2))
            pg = (hgrad[full, :] * slope).astype(bf16)
            pgr[full, :] = pg
            stats[8:9, :] += jnp.sum(pg.astype(f32), axis=0, keepdims=True)
        loop(8, act)
        part = dot(pgr[rows, :], w1[...], NT)

        @pl.when(i == 0)
        def _():
            own[...] = part

        @pl.when(i == 1)
        def _():
            rso[1] = part.astype(bf16)
            rs3.start(1)

        @pl.when(i == 2)
        def _():
            nbrf[...] = part

        @pl.when(i == 3)
        def _():
            rso[0] = part.astype(bf16)
            rs3.start(0)
    big = stage
    loop(4, mlp_block)
    ag3.finish()
    rs3.take(0)

    def nbr_rows(i):
        rows = pl.ds(pl.multiple_of(i * 32, 32), 32)
        rso[2, rows, :] = (nbrf[rows, :] + rsi[0, rows, :].astype(f32)).astype(bf16)
    loop(8, nbr_rows)
    rs3.start(2)

    rs2 = Scatter(at, rs2o, rs2i, sems, S_RS2)

    def out_block(i):
        rows = quarter(at.flip(at.rank, 3 - (((i & 1) << 1) | (i >> 1))))
        part = dot(hid[rows, :], w2[...], NN)

        @pl.when(i == 0)
        def _():
            rs2o[0] = part.astype(bf16)
            rs2.start(0)

        @pl.when(i == 1)
        def _():
            rs2.take(0)
            mlpz[...] = (part + rs2i[0].astype(f32)).astype(bf16)

        @pl.when(i == 2)
        def _():
            rs2o[1] = part.astype(bf16)
            rs2.start(1)

        @pl.when(i == 3)
        def _():
            rs2.take(1)
            mlpown[...] = part + rs2i[1].astype(f32)
    loop(4, out_block)
    rs2.copy(0).wait_send()
    rs2.copy(1).wait_send()
    rs3.take(1)
    rs3.take(2)

    def back_rows(i):
        rows = pl.ds(pl.multiple_of(i * 32, 32), 32)
        back = own[rows, :] + rsi[1, rows, :].astype(f32) + rsi[2, rows, :].astype(f32)
        normed = n2[rows, :]
        stats[3:4, :] += jnp.sum(back, axis=0, keepdims=True)
        stats[4:5, :] += jnp.sum(back * normed, axis=0, keepdims=True)
        u = back * (1.0 + mods[scale_mlp, :])
        mean_u = jnp.mean(u, axis=1, keepdims=True)
        mean_p = jnp.mean(u * normed, axis=1, keepdims=True)
        gout = cs[rows, :].astype(f32)
        mg = gout + (u - mean_u - normed * mean_p) * inv2[rows, 0:1]
        mgrad[rows, :] = mg
        ag = mods[gate_attn, :] * mg
        stats[2:3, :] += jnp.sum(mg * branch[rows, :], axis=0, keepdims=True)
        stats[6:7, :] += jnp.sum(ag, axis=0, keepdims=True)
        stats[7:8, :] += jnp.sum(mods[gate_mlp, :] * gout, axis=0, keepdims=True)
        target = pl.ds(pl.multiple_of(at.rank * 256 + i * 32, 32), 32)
        gr[target, :] = ag.astype(bf16)
    loop(8, back_rows)
    rs3.finish()
    ag4 = Gather(at, gr, sems, S_AG4)
    ag4.start()

    def wgrad(left, right, out, i):
        cols = pl.ds(pl.multiple_of(i * 128, 128), 128)
        tile = dot(left[:, cols], right[...], TN).astype(bf16)
        out[cols, :] = tile
    loop(9, lambda i: wgrad(mr, pgr, g1, i))
    loop(9, lambda i: wgrad(cr, hid, g2, i))
    ag4.take_sib()
    ag4.take_nbr()
    ag4.take_diag()
    ag4.finish()
    for_mods(lambda cp: cp.wait_send(), None)

    @pl.when(at.away)
    def _():
        send(tok, xs, sems, S_X, at.swap).wait_send()
        send(bblk, bias, sems, S_BIAS, at.swap).wait_send()
        send(cot, cr.at[quarter(at.r_sib)], sems, S_C, at.swap).wait_send()
        for i in range(10):
            import_first(i).wait_send()
            for k in range(3):
                import_next(i, k, at.c).wait_send()


def call_kf(*args):
    S, D, H = 1024, 1152, 288
    V = pltpu.VMEM
    outs = [((S, D), bf16), ((4, S, 128), bf16), ((4, S, 128), bf16), ((4, S, 128), bf16), ((4, 128, S), bf16), ((4, 8, S), f32),
            ((S, H), bf16), ((S, D), bf16), ((256, D), f32), ((256, D), bf16), ((256, D), bf16), ((256, D), f32), ((8, D), f32),
            ((16, D), f32), ((256, D), f32), ((256, D), bf16), ((D, D), bf16), ((D, D), bf16), ((3, D, H), bf16), ((H, D), bf16)]
    scratch = [V((D, D), bf16), V((D, D), bf16), V((4, 128, S), bf16), V((S, D), bf16), V((S, D), bf16), V((S, D), f32),
               V((S, D), bf16), V((S, D), bf16), V((3, 256, D), bf16), V((3, 256, D), bf16), V((256, D), f32), V((256, D), f32),
               V((2, 256, D), bf16), V((2, 256, D), bf16), V((256, D), f32), V((256, D), f32), V((4, 8, D), f32), V((8, D), f32),
               V((256, 384), f32), V((384, 256), f32), V((256, 128), f32), V((256, D), f32),
               pltpu.SemaphoreType.DMA((2, N_SEMS)), pltpu.SemaphoreType.DMA((4,))]
    vm, anys = pl.BlockSpec(memory_space=pltpu.VMEM), pl.BlockSpec(memory_space=pl.ANY)
    return pl.pallas_call(
        kf, name="front",
        out_shape=[jax.ShapeDtypeStruct(s, d) for s, d in outs],
        in_specs=[anys, anys, vm, vm, vm, anys, anys, anys, anys],
        out_specs=[vm] * len(outs), scratch_shapes=scratch,
        compiler_params=pltpu.CompilerParams(collective_id=1, has_side_effects=True, vmem_limit_bytes=67043328),
    )(*args)


T_Z, T_RS4, T_G, T_OUT, T_IG, T_FZ, T_SB, T_GS, T_AL = 0, 1, 4, 13, 14, 15, 21, 24, 27
N_BACK = 27 + 7
L_IN = 17


def kb(xr_h, qn_h, kn_h, vn_h, kt_h, lse_h, mix_h, gr_h, mgrad_h, xs_h, cs_h, mid_h, mods, stats_h, mlpown_h, mlpz, g1, g2, wq_h, wp_h,
       obias,
       out_o, ig_o, w1_o, w2_o, w4_o, al,
       xr, qn, kn, vn, kt, lse, mix, gr, mgrad, xs, cs, mid, stats, mlpown, wq, wp,
       don, dh, dense, dka, dva, rso, rsi, own, rs2z, g4, rg1, rg2, rg4, gown, half, half4, keep, keep4, fz, fz4, sb, sb4,
       outb, igb, acc, gs, lb, sems, lsem):
    at = Spot()
    inv_root = 1.0 / math.sqrt(HEAD_DIM)
    far = (at.dp, at.flip(at.z, 2))
    diag = (at.flip(at.dp, 1), at.flip(at.z, 1))
    spread = [*at.peers, far, *[(at.flip(at.dp, 2 * k), at.flip(at.z, 2)) for k in (1, 2, 3)]]
    entry(at, [far, diag, *spread[4:]])

    loads = [(gr_h, gr), (wp_h, wp), (kn_h, kn), (qn_h, qn), (vn_h, vn), (kt_h, kt), (lse_h, lse), (wq_h, wq), (xr_h, xr), (mix_h, mix),
             (mgrad_h, mgrad), (xs_h, xs), (cs_h, cs), (mid_h, mid), (stats_h, stats), (mlpown_h, mlpown)]
    for i, (a, b) in enumerate(loads):
        pltpu.make_async_copy(a, b, lsem.at[i]).start()

    def have(*indices):
        for i in indices:
            pltpu.make_async_copy(loads[i][0], loads[i][1], lsem.at[i]).wait()

    zcopy = send(mlpz, rs2z, sems, T_Z, at.nbr)
    zcopy.start()

    def slice_rows(slot, size=288):
        return pl.ds(pl.multiple_of(slot * size, 16), size)

    def gcopy(m, k):
        rows = slice_rows(at.flip(at.c, k + 1))
        if m == 2:
            return send(g4.at[:, rows, :], rg4.at[k], sems, T_G + 6 + k, at.peers[k])
        return send((g1, g2)[m].at[rows, :], (rg1, rg2)[m].at[k], sems, T_G + 3 * m + k, at.peers[k])

    for m in range(2):
        for k in range(3):
            gcopy(m, k).start()
        mine = pltpu.make_async_copy((g1, g2)[m].at[slice_rows(at.c), :], gown.at[m], lsem.at[16 + m])
        mine.start()

    have(0, 1)

    def mix_block(i):
        rows = quarter(i)
        acc[:, :288] = dot(gr[rows, :], wp[...], NT)

        def store(h, head):
            don[h, rows, :] = head.astype(bf16)
        split_heads(acc, store)
    loop(4, mix_block)
    have(2, 3, 4, 5, 6)

    def back_head(h):
        dka[...] = jnp.zeros(dka.shape, f32)
        dva[...] = jnp.zeros(dva.shape, f32)

        def back_block(i):
            rows = quarter(i)
            qb, db = qn[h, rows, :], don[h, rows, :]
            st = dot(kn[h], qb, NT)
            probs = jnp.exp(st * inv_root - lse[h, 0:1, rows])
            dp = dot(vn[h], db, NT)
            row = jnp.sum(probs * dp, axis=0, keepdims=True)
            ds = (probs * (dp - row)).astype(bf16)
            dqt = dot(kt[h], ds, NN) * inv_root
            dh[0, h, rows, :] = dqt.T.astype(bf16)
            dka[...] += dot(ds, qb, NN)
            dva[...] += dot(probs.astype(bf16), db, NN)
        loop(4, back_block)
        dh[1, h] = (dka[...] * inv_root).astype(bf16)
        dh[2, h] = dva[...].astype(bf16)
    loop(4, back_head)
    have(7)
    rs4 = Scatter(at, rso, rsi, sems, T_RS4)

    def back_part(i):
        rows = quarter(at.flip(at.rank, 3 - (((i & 1) << 1) | (i >> 1))))
        for t in range(3):
            dense[t, rows, :] = join_heads([dh[t, h, rows, :].astype(f32) for h in range(4)]).astype(bf16)
        part = dot(dense[0, rows, :], wq[0], NT)
        part += dot(dense[1, rows, :], wq[1], NT)
        part += dot(dense[2, rows, :], wq[2], NT)

        @pl.when(i == 0)
        def _():
            rso[0] = part.astype(bf16)
            rs4.start(0)

        @pl.when(i == 1)
        def _():
            rs4.take(0)
            rso[2] = (part + rsi[0].astype(f32)).astype(bf16)
            rs4.start(2)

        @pl.when(i == 2)
        def _():
            rso[1] = part.astype(bf16)
            rs4.start(1)

        @pl.when(i == 3)
        def _():
            own[...] = part
    loop(4, back_part)

    have(8, 9)

    def wgrad(i):
        cols = pl.ds(pl.multiple_of(i * 128, 128), 128)
        g4[0, cols, :] = dot(gr[:, cols], mix[...], TN).astype(bf16)
        for t in range(3):
            g4[1 + t, cols, :] = dot(xr[:, cols], dense[t], TN).astype(bf16)
    loop(9, wgrad)
    for k in range(3):
        gcopy(2, k).start()
    have(10, 11, 12, 13, 14, 15)
    for row, t in ((9, 0), (10, 2)):
        stats[row:row + 1, :288] = jnp.sum(dense[t].astype(f32), axis=0, keepdims=True)

    zcopy.wait_recv()
    gate_mlp = mods[5:6, :]

    def out_rows(i):
        rows = pl.ds(pl.multiple_of(i * 32, 32), 32)
        br = mlpown[rows, :] + rs2z[rows, :].astype(f32) + obias[1:2, :]
        stats[5:6, :] += jnp.sum(cs[rows, :].astype(f32) * br, axis=0, keepdims=True)
        outb[rows, :] = (mid[rows, :] + gate_mlp * br).astype(bf16)
    loop(8, out_rows)

    @pl.when(at.away)
    def _():
        send(outb, out_o, sems, T_OUT, at.swap).start()

    @pl.when(at.home)
    def _():
        out_o[...] = outb[...]

    rs4.take(1)
    rs4.take(2)
    scale_attn = mods[1:2, :]

    def in_rows(i):
        rows = pl.ds(pl.multiple_of(i * 32, 32), 32)
        back = own[rows, :] + rsi[1, rows, :].astype(f32) + rsi[2, rows, :].astype(f32)
        normed, inv = center_rows(xs[rows, :].astype(f32))
        stats[0:1, :] += jnp.sum(back, axis=0, keepdims=True)
        stats[1:2, :] += jnp.sum(back * normed, axis=0, keepdims=True)
        w = back * (1.0 + scale_attn)
        mean_w = jnp.mean(w, axis=1, keepdims=True)
        mean_p = jnp.mean(w * normed, axis=1, keepdims=True)
        total = mgrad[rows, :] + (w - mean_w - normed * mean_p) * inv
        ig_o[rows, :] = total
        igb[0, rows, :] = total.astype(bf16)
    loop(8, in_rows)

    @pl.when(at.away)
    def _():
        send(igb.at[0], igb.at[1], sems, T_IG, at.swap).start()

    gs[0] = stats[...]
    mates = [at.sib, at.nbr, diag]

    def gs_copy(k):
        return send(gs.at[0], gs.at[k + 1], sems, T_GS + k, mates[k])
    for k in range(3):
        gs_copy(k).start()

    def reduce_matrix(m):
        mine = pltpu.make_async_copy((g1, g2)[m].at[slice_rows(at.c), :], gown.at[m], lsem.at[16 + m])
        mine.wait()
        into = (rg1, rg2)[m]
        for k in range(3):
            send(gown.at[m], into.at[k], sems, T_G + 3 * m + k, at.peers[k]).wait_recv()

        def add(i):
            for h in range(2):
                rows = pl.ds(pl.multiple_of(h * 144 + i * 16, 16), 16)
                part = pl.ds(pl.multiple_of(i * 16, 16), 16)
                total = (gown[m, rows, :].astype(f32) + into[0, rows, :].astype(f32)
                         + into[1, rows, :].astype(f32) + into[2, rows, :].astype(f32))
                half[m, h, part, :] = total.astype(bf16)

                @pl.when(at.q == h)
                def _():
                    keep[m, part, :] = total
        loop(9, add)

    def reduce_last():
        for k in range(3):
            send(g4.at[:, slice_rows(at.c), :], rg4.at[k], sems, T_G + 6 + k, at.peers[k]).wait_recv()

        def add(i):
            for t in range(4):
                for h in range(2):
                    rows = pl.ds(pl.multiple_of(h * 144 + i * 16, 16), 16)
                    part = pl.ds(pl.multiple_of(i * 16, 16), 16)
                    full = pl.ds(pl.multiple_of(at.c * 288 + h * 144 + i * 16, 16), 16)
                    total = (g4[t, full, :].astype(f32) + rg4[0, t, rows, :].astype(f32)
                             + rg4[1, t, rows, :].astype(f32) + rg4[2, t, rows, :].astype(f32))
                    half4[h, t, part, :] = total.astype(bf16)

                    @pl.when(at.q == h)
                    def _():
                        keep4[t, part, :] = total
        loop(9, add)

    def home_copies(m, other, same):
        src = half4 if m == 2 else half.at[m]
        z_to, s_to = (fz4, sb4) if m == 2 else (fz.at[m], sb.at[m])
        return (send(src.at[other], s_to, sems, T_SB + m, at.sib),
                send(src.at[same], z_to, sems, T_FZ + m, far),
                send(src.at[other], z_to, sems, T_FZ + 3 + m, at.swap))

    def hand_home(m, what):
        to_sib, to_far, to_swap = home_copies(m, 1 - at.q, at.q)

        @pl.when(at.home)
        def _():
            what(to_sib)

        @pl.when(at.away)
        def _():
            what(to_far)
            what(to_swap)

    def arrive(m):
        to_sib, to_far, to_swap = home_copies(m, 1 - at.q, at.q)

        @pl.when(at.home)
        def _():
            to_far.wait_recv()

        @pl.when(at.away)
        def _():
            to_sib.wait_recv()
            to_swap.wait_recv()

    for m in range(2):
        reduce_matrix(m)
        hand_home(m, lambda cp: cp.start())

    for k in range(3):
        gs_copy(k).wait_recv()
    lb[0:8, :] = gs[0, 0:8, :] + gs[1, 0:8, :] + gs[2, 0:8, :] + gs[3, 0:8, :]
    for k, bits in enumerate((0, 2, 1, 3)):
        for rank in range(4):
            @pl.when(at.flip(at.rank, bits) == rank)
            def _():
                lb[8 + 3 * rank:11 + 3 * rank, :] = gs[k, 8:11, :]
    lb[20:22, :] = mods[6:8, :]
    latent = at.dp - at.q + at.g

    def al_copy(k):
        return send(lb, al.at[latent], sems, T_AL + k, spread[k])
    for k in range(7):
        al_copy(k).start()
    al[latent] = lb[...]

    reduce_last()
    hand_home(2, lambda cp: cp.start())
    for m in range(2):
        arrive(m)

        @pl.when(at.home)
        def _():
            (w1_o, w2_o)[m][...] = keep[m] + fz[m].astype(f32)

        @pl.when(at.away)
        def _():
            (w1_o, w2_o)[m][...] = sb[m].astype(f32) + fz[m].astype(f32)

    @pl.when(at.away)
    def _():
        send(outb, out_o, sems, T_OUT, at.swap).wait()
        send(igb.at[0], igb.at[1], sems, T_IG, at.swap).wait()

        def widen(i):
            rows = pl.ds(pl.multiple_of(i * 32, 32), 32)
            ig_o[rows, :] = igb[1, rows, :].astype(f32)
        loop(8, widen)
    arrive(2)

    @pl.when(at.home)
    def _():
        w4_o[...] = keep4[...] + fz4[...].astype(f32)

    @pl.when(at.away)
    def _():
        w4_o[...] = sb4[...].astype(f32) + fz4[...].astype(f32)
    for k in range(7):
        al_copy(k).wait_recv()
    zcopy.wait_send()
    rs4.finish()
    for m in range(3):
        for k in range(3):
            gcopy(m, k).wait_send()
        hand_home(m, lambda cp: cp.wait_send())
    for k in range(3):
        gs_copy(k).wait_send()
    for k in range(7):
        al_copy(k).wait_send()


def call_kb(*args):
    S, D, H = 1024, 1152, 288
    V = pltpu.VMEM
    outs = [((256, D), bf16), ((256, D), f32), ((144, D), f32), ((144, D), f32), ((4, 144, H), f32), ((8, 24, D), f32)]
    scratch = [V((S, D), bf16), V((4, S, 128), bf16), V((4, S, 128), bf16), V((4, S, 128), bf16), V((4, 128, S), bf16), V((4, 8, S), f32),
               V((S, H), bf16), V((S, D), bf16), V((256, D), f32), V((256, D), bf16), V((256, D), bf16), V((256, D), f32), V((16, D), f32),
               V((256, D), f32), V((3, D, H), bf16), V((H, D), bf16),
               V((4, S, 128), bf16), V((3, 4, S, 128), bf16), V((3, S, H), bf16), V((S, 128), f32), V((S, 128), f32),
               V((3, 256, D), bf16), V((3, 256, D), bf16), V((256, D), f32), V((256, D), bf16),
               V((4, D, H), bf16), V((3, H, D), bf16), V((3, H, D), bf16), V((3, 4, H, H), bf16), V((2, H, D), bf16),
               V((2, 2, 144, D), bf16), V((2, 4, 144, H), bf16), V((2, 144, D), f32), V((4, 144, H), f32),
               V((2, 144, D), bf16), V((4, 144, H), bf16), V((2, 144, D), bf16), V((4, 144, H), bf16),
               V((256, D), bf16), V((2, 256, D), bf16), V((256, 384), f32), V((4, 16, D), f32), V((24, D), f32),
               pltpu.SemaphoreType.DMA((2, N_BACK)), pltpu.SemaphoreType.DMA((18,))]
    vm, anys = pl.BlockSpec(memory_space=pltpu.VMEM), pl.BlockSpec(memory_space=pl.ANY)
    specs = [anys] * 12 + [vm] + [anys] * 2 + [anys] + [anys] * 4 + [vm]
    return pl.pallas_call(
        kb, name="back",
        out_shape=[jax.ShapeDtypeStruct(s, d) for s, d in outs],
        in_specs=specs, out_specs=[vm] * len(outs), scratch_shapes=scratch,
        compiler_params=pltpu.CompilerParams(collective_id=2, has_side_effects=True, vmem_limit_bytes=67043328),
    )(*args)


def kc(part, all_o, sems):
    at = Spot()
    barrier = pltpu.get_barrier_semaphore()
    mates = [(at.dp, at.flip(at.z, k)) for k in (1, 2, 3)]
    for mate in mates:
        pl.semaphore_signal(barrier, inc=1, device_id=mate, device_id_type=MESH)
    pl.semaphore_wait(barrier, 3)
    copies = [send(part, all_o.at[k + 1], sems, k, mates[k]) for k in range(3)]
    for cp in copies:
        cp.start()
    all_o[0] = part[...]
    for cp in copies:
        cp.wait()


def call_kc(part):
    vm = pl.BlockSpec(memory_space=pltpu.VMEM)
    return pl.pallas_call(
        kc, name="small", out_shape=jax.ShapeDtypeStruct((4, *part.shape), f32), in_specs=[vm], out_specs=vm,
        scratch_shapes=[pltpu.SemaphoreType.DMA((2, 3))],
        compiler_params=pltpu.CompilerParams(collective_id=3, has_side_effects=True),
    )(part)


def fast_body(tokens, labels, timesteps, label_table, ada_weight, ada_bias, qkv_weight, qv_bias, proj_weight, out_bias, fc1_weight,
              fc1_bias, fc2_weight, cotangent):
    width, cols = tokens.shape[2], ada_weight.shape[1]
    dp_rank, z_rank = lax.axis_index("dp"), lax.axis_index("tensor")
    cond = label_table[labels].astype(f32) + time_features(timesteps, width)
    cond_low = jax.nn.silu(cond).astype(bf16)
    mod = jnp.dot(cond_low, ada_weight, preferred_element_type=f32) + ada_bias
    third = cols // 3
    mblk = jnp.concatenate([
        jnp.pad(mod.reshape(3, third), ((0, 0), (0, width - third))), cond,
        jnp.broadcast_to(labels.astype(f32)[:, None], (1, width)), jnp.zeros((3, width), f32)])
    bblk = jnp.concatenate([fc1_bias[None], jnp.pad(qv_bias, ((0, 0), (0, width - qv_bias.shape[1]))), jnp.zeros((5, width), f32)])
    front = call_kf(tokens[0], cotangent[0], mblk, bblk, out_bias, qkv_weight, proj_weight, fc1_weight, fc2_weight)
    output, input_grad, w1, w2, w4, al = call_kb(*front, out_bias)
    mod_all = al[:, :6].reshape(8, 6 * width)
    mod_cols = lax.dynamic_slice_in_dim(mod_all, z_rank * cols, cols, 1)
    terms = jnp.dot(mod_cols, ada_weight.astype(f32).T, precision=lax.Precision.HIGHEST)
    silu_grad = jnp.sum(call_kc(terms), axis=0)
    cond_all, label_all = al[:, 20], al[:, 21, 0].astype(jnp.int32)
    low_all, silu_pull = jax.vjp(jax.nn.silu, cond_all)
    cond_grad = silu_pull(silu_grad)[0]
    low_all = low_all.astype(bf16).astype(f32)
    rows = width // lax.axis_size("dp")
    low_rows = lax.dynamic_slice_in_dim(low_all, dp_rank * rows, rows, 1)
    ada_grad = sum(low_rows[n][:, None] * mod_cols[n][None, :] for n in range(8))
    ada_bias_grad = lax.dynamic_slice_in_dim(jnp.sum(mod_cols, axis=0), dp_rank * (cols // 8), cols // 8, 0)
    class_ids = jnp.arange(label_table.shape[0], dtype=jnp.int32)
    table_grad = sum(jnp.where((class_ids == label_all[n])[:, None], cond_grad[n][None, :], 0.0) for n in range(8))
    sums = jnp.sum(al, axis=0)
    out_bias_grad = sums[6:8]
    ranks = sums[8:20].reshape(4, 3, width)
    qv_grad = jnp.moveaxis(ranks[:, 1:3, :width // 4], 0, 1).reshape(2, width)
    fc1_bias_grad = lax.dynamic_slice(ranks[:, 0], (z_rank, dp_rank * rows), (1, rows))[0]
    return (output[None], input_grad[None], table_grad, ada_grad, ada_bias_grad, w4[1:], qv_grad, w4[0].T, out_bias_grad, w1, fc1_bias_grad, w2.T)


def solution(mesh):
    placed = (
        P("dp", "tensor", None),
        P("dp"),
        P("dp"),
        P(),
        P(None, "tensor"),
        P("tensor"),
        P(None, None, "tensor"),
        P(None, "tensor"),
        P("tensor", None),
        P(),
        P(None, "tensor"),
        P("tensor"),
        P("tensor", None),
        P("dp", "tensor", None),
    )
    small = mesh.shape["dp"] == 8 and mesh.shape["tensor"] == 4
    return jax.shard_map(
        fast_body if small else body,
        mesh=mesh,
        in_specs=placed,
        out_specs=(
            P("dp", "tensor", None),
            P("dp", "tensor", None),
            P(),
            P("dp", "tensor"),
            P(("tensor", "dp")),
            P(None, "dp", "tensor"),
            P(),
            P("tensor", "dp"),
            P(),
            P("dp", "tensor"),
            P(("tensor", "dp")),
            P("tensor", "dp"),
        ),
        check_vma=False,
    )
```
